32 devices in a mesh: dp: 4 (over z), seq: 2 (over x), tensor: 4 (over y, core).
Axes of the slice: x: 2, y: 2, z: 4, core: 2. Of those that a mesh axis runs over, the one named last changes fastest.
Arguments:
- latents: bfloat16 [4, 4, 256, 1152], P('dp', 'seq', 'tensor'), may hold values from -6 to 6
- modulation: float32 [4, 6, 1152], P('dp'), may hold values from -3 to 3
- in_weight: bfloat16 [1152, 3, 1152], P(None, None, 'tensor'), may hold values from -0.5 to 0.5
- out_weight: bfloat16 [1152, 1152], P('tensor'), may hold values from -0.1875 to 0.1875
- up_weight: bfloat16 [1152, 4608], P(None, 'tensor'), may hold values from -0.1875 to 0.1875
- down_weight: bfloat16 [4608, 1152], P('tensor'), may hold values from -0.09375 to 0.09375
- cotangent: bfloat16 [4, 4, 256, 1152], P('dp', 'seq', 'tensor'), may hold values from -6 to 6
Outputs:
- result: bfloat16 [4, 4, 256, 1152], P('dp', 'seq', 'tensor')
- latents_grad: bfloat16 [4, 4, 256, 1152], P('dp', 'seq', 'tensor')
- in_grad: bfloat16 [1152, 3, 1152], P(('dp', 'seq'), None, 'tensor')
- out_grad: bfloat16 [1152, 1152], P('tensor', ('dp', 'seq'))
- up_grad: bfloat16 [1152, 4608], P(('dp', 'seq'), 'tensor')
- down_grad: bfloat16 [4608, 1152], P('tensor', ('dp', 'seq'))
The draws below stay inside these ranges and needn't reach their ends.
All inputs are finite; a program needn't handle non-finite values.
Results may differ from the reference program's by a relative error of at most 0.02.
The reference program's roundings to bfloat16 on the way count: a program that leaves them out, or rounds other values in their place, can miss the bound.
Values may be sent and summed in bfloat16 or wider, within the bound.
A program may use at most 128 MiB of HBM per device.

```python
import math
import jax
import jax.numpy as jnp
from jax import lax

D = 1152
HEADS = 16
FF = 4608
PIX = 256
FRAMES = 4
BATCH = 4


def draw_latents(key, part):
    shape = (BATCH, FRAMES, PIX, D)
    values = jax.random.normal(key, shape, jnp.float32)
    return jnp.clip(values, -6.0, 6.0).astype(jnp.bfloat16)


def draw_in_weight(key, part):
    first_key = jax.random.fold_in(key, 0)
    basis = jax.random.normal(first_key, (D, 3, D), jnp.float32) * D ** (-0.5)
    values = basis
    return jnp.clip(values, -0.5, 0.5).astype(jnp.bfloat16)


def with_spikes(values, rng, source, target, shards_of, factor):
    def block_of(position):
        return (jnp.arange(values.shape[position]) // (values.shape[position] // shards_of)).reshape((-1,) + (1,) * (values.ndim - 1 - position))

    one_side = jax.random.permutation(rng, shards_of)[block_of(target)]
    far = (block_of(target) + shards_of // 2) % shards_of
    return jnp.where((block_of(source) == one_side) | (block_of(source) == far), factor * values, values)


def level_of(stream_key, shape, cuts, least, largest):
    gain = 1.0
    for axis_at, blocks in cuts:
        draws = jax.random.uniform(jax.random.fold_in(jax.random.fold_in(stream_key, 6), axis_at), (blocks,), jnp.float32, least / len(cuts), largest / len(cuts))
        gain = gain * jnp.repeat(jnp.exp(draws), shape[axis_at] // blocks).reshape((-1,) + (1,) * (len(shape) - 1 - axis_at))
    return gain


def gaussian(own_key, extent, scale, reach, cuts=(), kind=jnp.bfloat16):
    values = scale * jax.random.normal(own_key, extent, jnp.float32)
    if cuts:
        values = values * level_of(own_key, extent, cuts, -0.22, 0.18)
    return jnp.clip(values, -reach, reach).astype(kind)


def gaussian_with(rng, extent, scale, limit, cuts, heavy, dtype=jnp.bfloat16):
    entries = scale * jax.random.normal(rng, extent, jnp.float32)
    if cuts:
        entries = entries * level_of(rng, extent, cuts, -0.22, 0.18)
    return jnp.clip(with_spikes(entries, jax.random.fold_in(rng, 3), *heavy), -limit, limit).astype(dtype)


def setup_inputs(seed: int = 0) -> dict:
    keys = jax.random.split(jax.random.key(seed), 8)
    latents = draw_latents(jax.random.fold_in(keys[7], 71), 0)
    modulation = gaussian(keys[1], (BATCH, 6, D), 0.5, 3.0, ((0, 4),), jnp.float32)
    in_weight = draw_in_weight(jax.random.fold_in(keys[7], 71), 0)
    out_weight = gaussian(keys[3], (D, D), D ** -0.5, 0.1875, ((0, 4),))
    up_weight = gaussian(keys[4], (D, FF), D ** -0.5, 0.1875, ((1, 4),))
    down_weight = gaussian(keys[5], (FF, D), FF ** -0.5, 0.09375, ((0, 4),))
    cotangent = gaussian_with(keys[6], (BATCH, FRAMES, PIX, D), 1.0, 6.0, ((0, 4), (1, 2), (2, 4)), (1, 3, 2, 2.0))
    return {"latents": latents, "modulation": modulation, "in_weight": in_weight, "out_weight": out_weight, "up_weight": up_weight, "down_weight": down_weight, "cotangent": cotangent}


epsilon = 1e-06

def normalize(rows):
    center = lax.optimization_barrier(jnp.mean(rows, axis=-1, keepdims=True))
    centred = rows - center
    spread = lax.optimization_barrier(jnp.mean(centred * centred, axis=-1, keepdims=True))
    inverse = lax.rsqrt(spread + epsilon)
    return (centred * inverse, inverse)

def norm_back(normed, inverse, upstream):
    mean_grad = lax.optimization_barrier(jnp.mean(upstream, axis=-1, keepdims=True))
    mean_cross = lax.optimization_barrier(jnp.mean(upstream * normed, axis=-1, keepdims=True))
    return (upstream - mean_grad - normed * mean_cross) * inverse

def gelu_tanh(values):
    return jax.nn.gelu(values, approximate=True)

def flat_dot(left, right):
    leading = left.shape[:-1]
    out_rows = jnp.dot(left.reshape(-1, left.shape[-1]), right, preferred_element_type=jnp.float32)
    return out_rows.reshape(leading + (right.shape[-1],))

def flat_dot_t(left, right):
    leading = left.shape[:-1]
    out_rows = lax.dot_general(left.reshape(-1, left.shape[-1]), right, (((1,), (1,)), ((), ())), preferred_element_type=jnp.float32)
    return out_rows.reshape(leading + (right.shape[0],))

def weight_grad(left, right):
    return lax.dot_general(left.reshape(-1, left.shape[-1]), right.reshape(-1, right.shape[-1]), (((0,), (0,)), ((), ())), preferred_element_type=jnp.float32)

def attend(queries, key_rows, value_rows):
    scaling = 1.0 / math.sqrt(queries.shape[-1])
    scores = jnp.einsum('bfphe,bgphe->bphfg', queries.astype(jnp.float32), key_rows.astype(jnp.float32)) * scaling
    highest = lax.optimization_barrier(jnp.max(scores, axis=-1, keepdims=True))
    raised = jnp.exp(scores - highest)
    probs = raised / lax.optimization_barrier(jnp.sum(raised, axis=-1, keepdims=True))
    probs_low = probs.astype(jnp.bfloat16)
    attended = jnp.einsum('bphfg,bgphe->bfphe', probs_low.astype(jnp.float32), value_rows.astype(jnp.float32)).astype(jnp.bfloat16)
    return (attended, probs, probs_low)

def attend_back(queries, key_rows, value_rows, probs, probs_low, attended_grad):
    scaling = 1.0 / math.sqrt(queries.shape[-1])
    grad_wide = attended_grad.astype(jnp.float32)
    value_grad = jnp.einsum('bphfg,bfphe->bgphe', probs_low.astype(jnp.float32), grad_wide).astype(jnp.bfloat16)
    prob_grad = jnp.einsum('bfphe,bgphe->bphfg', grad_wide, value_rows.astype(jnp.float32))
    score_grad = probs * (prob_grad - lax.optimization_barrier(jnp.sum(probs * prob_grad, axis=-1, keepdims=True))) * scaling
    score_low = score_grad.astype(jnp.bfloat16).astype(jnp.float32)
    query_grad = jnp.einsum('bphfg,bgphe->bfphe', score_low, key_rows.astype(jnp.float32)).astype(jnp.bfloat16)
    key_grad = jnp.einsum('bphfg,bfphe->bgphe', score_low, queries.astype(jnp.float32)).astype(jnp.bfloat16)
    return (query_grad, key_grad, value_grad)

def reference(latents, modulation, in_weight, out_weight, up_weight, down_weight, cotangent):
    samples, frames_all, patches, width = latents.shape
    modulate = modulation[:, :, None, None, :]
    shift_first, scale_first, gate_first = (modulate[:, 0], modulate[:, 1], modulate[:, 2])
    shift_second, scale_second, gate_second = (modulate[:, 3], modulate[:, 4], modulate[:, 5])
    inputs = latents.astype(jnp.float32)
    first_normed, first_inverse = normalize(inputs)
    first_input = (first_normed * (1.0 + scale_first) + shift_first).astype(jnp.bfloat16)
    in_flat = in_weight.reshape(width, 3 * width)
    projected = flat_dot(first_input, in_flat).astype(jnp.bfloat16)
    split_parts = projected.reshape(samples, frames_all, patches, 3, HEADS, width // HEADS)
    queries, key_rows, value_rows = (split_parts[:, :, :, 0], split_parts[:, :, :, 1], split_parts[:, :, :, 2])
    attended, probs, probs_low = attend(queries, key_rows, value_rows)
    attended_flat = attended.reshape(samples, frames_all, patches, width)
    midway = inputs + gate_first * flat_dot(attended_flat, out_weight)
    second_normed, second_inverse = normalize(midway)
    second_input = (second_normed * (1.0 + scale_second) + shift_second).astype(jnp.bfloat16)
    hidden = flat_dot(second_input, up_weight)
    activated = gelu_tanh(hidden).astype(jnp.bfloat16)
    result = (midway + gate_second * flat_dot(activated, down_weight)).astype(jnp.bfloat16)
    upstream = cotangent.astype(jnp.float32)
    branch_grad = (gate_second * upstream).astype(jnp.bfloat16)
    down_grad = weight_grad(activated, branch_grad)
    activated_grad = flat_dot_t(branch_grad, down_weight)
    hidden_grad = jax.vjp(gelu_tanh, hidden)[1](activated_grad)[0].astype(jnp.bfloat16)
    up_grad = weight_grad(second_input, hidden_grad)
    second_grad = flat_dot_t(hidden_grad, up_weight)
    midway_grad = upstream + norm_back(second_normed, second_inverse, second_grad * (1.0 + scale_second))
    attention_grad = (gate_first * midway_grad).astype(jnp.bfloat16)
    out_grad = weight_grad(attended_flat, attention_grad)
    attended_grad = flat_dot_t(attention_grad, out_weight).astype(jnp.bfloat16)
    attended_grad = attended_grad.reshape(samples, frames_all, patches, HEADS, width // HEADS)
    query_grad, key_grad, value_grad = attend_back(queries, key_rows, value_rows, probs, probs_low, attended_grad)
    projected_grad = jnp.stack([query_grad, key_grad, value_grad], axis=3).reshape(samples, frames_all, patches, 3 * width)
    in_grad = weight_grad(first_input, projected_grad).reshape(width, 3, width)
    first_grad = flat_dot_t(projected_grad, in_flat)
    latents_grad = (midway_grad + norm_back(first_normed, first_inverse, first_grad * (1.0 + scale_first))).astype(jnp.bfloat16)
    return (result, latents_grad, in_grad.astype(jnp.bfloat16), out_grad.astype(jnp.bfloat16), up_grad.astype(jnp.bfloat16), down_grad.astype(jnp.bfloat16))
```

```python
import functools
import math

import jax
import jax.numpy as jnp
from jax import lax
from jax.experimental import pallas as pl
from jax.experimental.pallas import tpu as pltpu
from jax.sharding import PartitionSpec as P

HEAD_DIM = 72
epsilon = 1e-06
MESH = pl.DeviceIdType.MESH
F32 = jnp.float32
BF16 = jnp.bfloat16


def normalize(rows):
    center = jnp.mean(rows, axis=-1, keepdims=True)
    centred = rows - center
    spread = jnp.mean(centred * centred, axis=-1, keepdims=True)
    inverse = lax.rsqrt(spread + epsilon)
    return (centred * inverse, inverse)


def norm_back(normed, inverse, upstream):
    mean_grad = jnp.mean(upstream, axis=-1, keepdims=True)
    mean_cross = jnp.mean(upstream * normed, axis=-1, keepdims=True)
    return (upstream - mean_grad - normed * mean_cross) * inverse


def dot(left, right):
    return jnp.dot(left, right, preferred_element_type=F32)


def dot_t(left, right):
    return lax.dot_general(left, right, (((1,), (1,)), ((), ())), preferred_element_type=F32)


def head_sums(product, same_head):
    high = product.astype(BF16)
    low = (product - high.astype(F32)).astype(BF16)
    return dot(high, same_head) + dot(low, same_head)


def kernel(dims, lat, mod, in_w, out_w, up_w, down_w, cot, same_head,
           res_out, lgrad_out, gin_out, gout_out, gup_out, gdown_out,
           LAT, COT, FIRST, BRANCH, SECOND, ATTG, QKV, DQKV, ATT, DACT, ACT, HG, XT, PART, keep,
           MID, MIDG, RESB, RESR, LGB, LGR, rsA, rsB, rsC, rsD,
           gdown, gup, gout, gin, ssem, rsem):
    Z, S, T, Fl, Pb, D, H, K = dims
    O = T // 2
    Fr = Fl * S
    R = Fr * Pb
    N = T * R
    z, s, t = lax.axis_index("dp"), lax.axis_index("seq"), lax.axis_index("tensor")
    o, inner = t // 2, lax.rem(t, 2)
    partner = {"tensor": o * 2 + 1 - inner}

    def outer(k):
        return lax.rem(o + k, O)

    def seq_peer(k):
        return lax.rem(s + k, S)

    def dp_peer(k):
        return lax.rem(z + k, Z)

    sends = []

    def send(src, dst, device):
        i = len(sends)
        copy = pltpu.make_async_remote_copy(
            src_ref=src, dst_ref=dst, send_sem=ssem.at[i], recv_sem=rsem.at[i],
            device_id=device, device_id_type=MESH)
        copy.start()
        sends.append(copy)
        return copy

    barrier = pltpu.get_barrier_semaphore()
    peers = [partner]
    peers += [{"tensor": outer(k) * 2 + inner} for k in range(1, O)]
    peers += [{"seq": seq_peer(k)} for k in range(1, S)]
    peers += [{"dp": dp_peer(k)} for k in range(1, Z)]
    for peer in peers:
        pl.semaphore_signal(barrier, inc=1, device_id=peer, device_id_type=MESH)
    pl.semaphore_wait(barrier, len(peers))

    def row(i):
        return mod[i : i + 1, :]

    def exchange_in(src, dst):
        copies = []
        for k in range(1, S):
            p = seq_peer(k)
            copies.append(send(src.at[:, p], dst.at[pl.ds(s * Fl, Fl)], {"seq": p}))
        dst[pl.ds(s * Fl, Fl)] = src[:, s]
        return copies

    def exchange_out(src, landed):
        copies = []
        for k in range(1, S):
            p = seq_peer(k)
            copies.append(send(src.at[pl.ds(p * Fl, Fl)], landed.at[k - 1], {"seq": p}))
        return copies

    def exchange_end(src, landed, out, copies):
        out[:, s] = src[pl.ds(s * Fl, Fl)]
        for k in range(1, S):
            copies[k - 1].wait_recv()
            out[:, lax.rem(s + S - k, S)] = landed[k - 1]

    def gather_start(buf):
        far = [send(buf.at[t], buf.at[t], {"tensor": outer(k) * 2 + inner}) for k in range(1, O)]
        near = [send(buf.at[t], buf.at[t], partner)]
        return far, near

    def gather_end(buf, state):
        far, near = state
        for k in range(1, O):
            far[k - 1].wait_recv()
            slot = lax.rem(o + O - k, O) * 2 + inner
            near.append(send(buf.at[slot], buf.at[slot], partner))
        for copy in near:
            copy.wait_recv()

    def scatter_start(compute, bufs):
        send1, recv1, send2, recv2 = bufs
        first = {}
        for k in list(range(1, O)) + [0]:
            PART[...] = compute(outer(k)).reshape(2, R, D)
            send1[k] = PART[1 - inner].astype(BF16)
            first[k] = send(send1.at[k], recv1.at[k], partner)
            keep[k] = PART[inner]
        second = []
        for k in range(1, O):
            first[k].wait_recv()
            send2[k - 1] = (keep[k] + recv1[k].astype(F32)).astype(BF16)
            second.append(send(send2.at[k - 1], recv2.at[k - 1], {"tensor": outer(k) * 2 + inner}))
        return first[0], second

    def scatter_end(bufs, state):
        send1, recv1, send2, recv2 = bufs
        state[0].wait_recv()
        total = keep[0] + recv1[0].astype(F32)
        for k in range(1, O):
            state[1][k - 1].wait_recv()
            total = total + recv2[k - 1].astype(F32)
        return total

    def pair(buf, i):
        both = buf[pl.ds(2 * i, 2)]
        return both.reshape(2 * R, both.shape[-1])

    def put_pair(buf, i, value):
        buf[pl.ds(2 * i, 2)] = value.reshape(2, R, value.shape[-1])

    def over_pairs(fn):
        def step(i, carry):
            fn(i)
            return carry
        lax.fori_loop(0, O, step, 0)

    def transpose_of(buf):
        for i in range(T):
            block = buf[i].T
            XT[:, :, i * R : (i + 1) * R] = block.reshape(Z, D // Z, R)

    def weight_start(right, bufs):
        local, rx, pz, rz = bufs
        def step(i, carry):
            value = dot(XT[i], right()).astype(BF16)
            local[i] = value.reshape(S, D // (Z * S), value.shape[-1])
            return carry
        lax.fori_loop(0, Z, step, 0)
        return [send(local.at[:, seq_peer(k)], rx.at[k - 1], {"seq": seq_peer(k)})
                for k in range(1, S)]

    def weight_mid(bufs, copies):
        local, rx, pz, rz = bufs
        for copy in copies:
            copy.wait_recv()
        def step(i, carry):
            total = local[i, s].astype(F32)
            for k in range(1, S):
                total = total + rx[k - 1, i].astype(F32)
            pz[i] = total.astype(BF16)
            return carry
        lax.fori_loop(0, Z, step, 0)
        return [send(pz.at[dp_peer(k)], rz.at[k - 1], {"dp": dp_peer(k)}) for k in range(1, Z)]

    def weight_end(bufs, copies):
        local, rx, pz, rz = bufs
        total = pz[z].astype(F32)
        for k in range(1, Z):
            copies[k - 1].wait_recv()
            total = total + rz[k - 1].astype(F32)
        return total.astype(BF16)

    lat_in = exchange_in(lat, LAT)
    cot_in = exchange_in(cot, COT)
    for copy in lat_in:
        copy.wait_recv()
    inputs = LAT[...].reshape(R, D).astype(F32)
    first_normed, first_inverse = normalize(inputs)
    FIRST[t] = (first_normed * (1.0 + row(1)) + row(0)).astype(BF16)
    first_state = gather_start(FIRST)
    for copy in cot_in:
        copy.wait_recv()
    BRANCH[t] = (row(5) * COT[...].reshape(R, D).astype(F32)).astype(BF16)
    branch_state = gather_start(BRANCH)
    gather_end(FIRST, first_state)

    def project(i):
        rows = pair(FIRST, i)
        for j in range(3):
            put_pair(QKV.at[j], i, dot(rows, in_w[j]).astype(BF16))
    over_pairs(project)

    scaling = 1.0 / math.sqrt(HEAD_DIM)

    def part(buf, j, i):
        return buf[j, i].astype(F32).reshape(Fr, Pb, H)

    def probabilities(q, k):
        scores = [head_sums((q * k[g : g + 1]).reshape(R, H), same_head[...]) * scaling for g in range(Fr)]
        highest = functools.reduce(jnp.maximum, scores)
        raised = [jnp.exp(score - highest) for score in scores]
        total = functools.reduce(jnp.add, raised)
        return [value / total for value in raised]

    def low(value):
        return value.astype(BF16).astype(F32)

    def attention(i, carry):
        q, k, v = part(QKV, 0, i), part(QKV, 1, i), part(QKV, 2, i)
        probs = probabilities(q, k)
        total = jnp.zeros((Fr, Pb, H), F32)
        for g in range(Fr):
            total = total + low(probs[g]).reshape(Fr, Pb, H) * v[g : g + 1]
        ATT[i] = total.reshape(R, H).astype(BF16)
        return carry
    lax.fori_loop(0, T, attention, 0)

    att_state = scatter_start(lambda i: dot(pair(ATT, i), out_w[...]), rsA)
    gather_end(BRANCH, branch_state)

    def branch_back(i):
        put_pair(DACT, i, dot_t(pair(BRANCH, i), down_w[...]))
    over_pairs(branch_back)
    midway = LAT[...].reshape(R, D).astype(F32) + row(2) * scatter_end(rsA, att_state)
    MID[...] = midway
    second_normed, second_inverse = normalize(midway)
    SECOND[t] = (second_normed * (1.0 + row(4)) + row(3)).astype(BF16)
    second_state = gather_start(SECOND)
    transpose_of(BRANCH)
    gather_end(SECOND, second_state)

    c = math.sqrt(2.0 / math.pi)

    def mlp(i):
        hidden = dot(pair(SECOND, i), up_w[...])
        square = hidden * hidden
        curve = jnp.tanh(c * (hidden + 0.044715 * square * hidden))
        put_pair(ACT, i, (0.5 * hidden * (1.0 + curve)).astype(BF16))
        slope = 0.5 * (1.0 + curve) + 0.5 * hidden * (1.0 - curve * curve) * (c * (1.0 + 3 * 0.044715 * square))
        put_pair(HG, i, (pair(DACT, i) * slope).astype(BF16))
    over_pairs(mlp)

    second_grad_state = scatter_start(lambda i: dot_t(pair(HG, i), up_w[...]), rsB)
    down_x = weight_start(lambda: ACT[...].reshape(N, K), gdown)
    second_grad = scatter_end(rsB, second_grad_state)
    second_normed, second_inverse = normalize(MID[...])
    midway_grad = COT[...].reshape(R, D).astype(F32) + norm_back(
        second_normed, second_inverse, second_grad * (1.0 + row(4)))
    MIDG[...] = midway_grad
    ATTG[t] = (row(2) * midway_grad).astype(BF16)
    attg_state = gather_start(ATTG)
    transpose_of(SECOND)
    up_x = weight_start(lambda: HG[...].reshape(N, K), gup)
    gather_end(ATTG, attg_state)

    def attention_back(i, carry):
        q, k, v = part(QKV, 0, i), part(QKV, 1, i), part(QKV, 2, i)
        grad = dot_t(ATTG[i], out_w[...]).astype(BF16).astype(F32).reshape(Fr, Pb, H)
        probs = probabilities(q, k)
        prob_grads = [head_sums((grad * v[g : g + 1]).reshape(R, H), same_head[...]) for g in range(Fr)]
        cross = functools.reduce(jnp.add, [a * b for a, b in zip(probs, prob_grads)])
        dq = jnp.zeros((Fr, Pb, H), F32)
        for g in range(Fr):
            score = low(probs[g] * (prob_grads[g] - cross) * scaling).reshape(Fr, Pb, H)
            dq = dq + score * k[g : g + 1]
            DQKV[1, i, g * Pb : (g + 1) * Pb] = jnp.sum(score * q, axis=0).astype(BF16)
            DQKV[2, i, g * Pb : (g + 1) * Pb] = jnp.sum(
                low(probs[g]).reshape(Fr, Pb, H) * grad, axis=0).astype(BF16)
        DQKV[0, i] = dq.reshape(R, H).astype(BF16)
        return carry
    lax.fori_loop(0, T, attention_back, 0)

    def first_back(i):
        return sum(dot_t(pair(DQKV.at[j], i), in_w[j]) for j in range(3))
    first_grad_state = scatter_start(first_back, rsC)
    transpose_of(FIRST)
    in_x = [weight_start(lambda j=j: DQKV[j].reshape(N, H), gin[j]) for j in range(3)]
    first_grad = scatter_end(rsC, first_grad_state)
    first_normed, first_inverse = normalize(LAT[...].reshape(R, D).astype(F32))
    LGB[...] = (MIDG[...] + norm_back(first_normed, first_inverse, first_grad * (1.0 + row(1)))
                ).astype(BF16).reshape(Fr, Pb, D)
    lgrad_copies = exchange_out(LGB, LGR)

    result_state = scatter_start(lambda i: dot(pair(ACT, i), down_w[...]), rsD)
    transpose_of(ATTG)
    out_x = weight_start(lambda: ATT[...].reshape(N, H), gout)
    down_z = weight_mid(gdown, down_x)
    feedforward = scatter_end(rsD, result_state)
    RESB[...] = (MID[...] + row(5) * feedforward).astype(BF16).reshape(Fr, Pb, D)
    res_copies = exchange_out(RESB, RESR)
    up_z = weight_mid(gup, up_x)
    in_z = [weight_mid(gin[j], in_x[j]) for j in range(3)]
    exchange_end(LGB, LGR, lgrad_out, lgrad_copies)
    out_z = weight_mid(gout, out_x)
    exchange_end(RESB, RESR, res_out, res_copies)
    gdown_out[...] = weight_end(gdown, down_z)
    gup_out[...] = weight_end(gup, up_z)
    for j in range(3):
        gin_out[j] = weight_end(gin[j], in_z[j])
    gout_out[...] = weight_end(gout, out_z)
    for copy in sends:
        copy.wait_send()


def body(sizes, latents, modulation, in_weight, out_weight, up_weight, down_weight, cotangent):
    Z, S, T = sizes
    _, Fl, Pl, D = latents.shape
    H, K = out_weight.shape[0], up_weight.shape[1]
    Pb, O = Pl // S, T // 2
    Fr = Fl * S
    R = Fr * Pb
    chunk = D // (Z * S)
    heads = jnp.arange(H) // HEAD_DIM
    same_head = (heads[:, None] == heads[None, :]).astype(BF16)

    def scatter_bufs():
        return (pltpu.VMEM((O, R, D), BF16), pltpu.VMEM((O, R, D), BF16),
                pltpu.VMEM((O - 1, R, D), BF16), pltpu.VMEM((O - 1, R, D), BF16))

    def weight_bufs(cols):
        return (pltpu.VMEM((Z, S, chunk, cols), BF16), pltpu.VMEM((S - 1, Z, chunk, cols), BF16),
                pltpu.VMEM((Z, chunk, cols), BF16), pltpu.VMEM((Z - 1, chunk, cols), BF16))

    full = pltpu.VMEM((T, R, D), BF16)
    tokens = pltpu.VMEM((Fr, Pb, D), BF16)
    landed = pltpu.VMEM((S - 1, Fl, Pb, D), BF16)
    copies = 2 * 4 * (S - 1 + O) + 4 * 2 * O + 6 * (S + Z)
    scratch = [
        tokens, tokens, full, full, full, full,
        pltpu.VMEM((3, T, R, H), BF16), pltpu.VMEM((3, T, R, H), BF16),
        pltpu.VMEM((T, R, H), BF16), pltpu.VMEM((T, R, K), F32),
        pltpu.VMEM((T, R, K), BF16), pltpu.VMEM((T, R, K), BF16),
        pltpu.VMEM((Z, D // Z, T * R), BF16), pltpu.VMEM((2, R, D), F32),
        pltpu.VMEM((O, R, D), F32),
        pltpu.VMEM((R, D), F32), pltpu.VMEM((R, D), F32),
        tokens, landed, tokens, landed,
        scatter_bufs(), scatter_bufs(), scatter_bufs(), scatter_bufs(),
        weight_bufs(K), weight_bufs(K), weight_bufs(H), tuple(weight_bufs(H) for _ in range(3)),
        pltpu.SemaphoreType.DMA((copies,)), pltpu.SemaphoreType.DMA((copies,)),
    ]
    vmem = pl.BlockSpec(memory_space=pltpu.VMEM)
    shape = jax.ShapeDtypeStruct
    outs = pl.pallas_call(
        functools.partial(kernel, (Z, S, T, Fl, Pb, D, H, K)),
        out_shape=(
            shape((Fl, S, Pb, D), BF16), shape((Fl, S, Pb, D), BF16),
            shape((3, chunk, H), BF16), shape((chunk, H), BF16),
            shape((chunk, K), BF16), shape((chunk, K), BF16)),
        in_specs=[vmem] * 8,
        out_specs=(vmem,) * 6,
        scratch_shapes=scratch,
        compiler_params=pltpu.CompilerParams(
            collective_id=0, has_side_effects=True, vmem_limit_bytes=67043328),
    )(latents.reshape(Fl, S, Pb, D), modulation[0], in_weight.transpose(1, 0, 2), out_weight,
      up_weight, down_weight, cotangent.reshape(Fl, S, Pb, D), same_head)
    res, lgrad, gin, gout, gup, gdown = outs
    return (res.reshape(1, Fl, Pl, D), lgrad.reshape(1, Fl, Pl, D), gin.transpose(1, 0, 2),
            gout.T, gup, gdown.T)


def solution(mesh):
    placed = (
        P("dp", "seq", "tensor", None),
        P("dp", None, None),
        P(None, None, "tensor"),
        P("tensor", None),
        P(None, "tensor"),
        P("tensor", None),
        P("dp", "seq", "tensor", None),
    )
    sizes = (mesh.shape["dp"], mesh.shape["seq"], mesh.shape["tensor"])
    return jax.shard_map(
        functools.partial(body, sizes),
        mesh=mesh,
        in_specs=placed,
        out_specs=(
            P("dp", "seq", "tensor", None),
            P("dp", "seq", "tensor", None),
            P(("dp", "seq"), None, "tensor"),
            P("tensor", ("dp", "seq")),
            P(("dp", "seq"), "tensor"),
            P("tensor", ("dp", "seq")),
        ),
        check_vma=False,
    )
```

```python
import functools
import math

import jax
import jax.numpy as jnp
from jax import lax
from jax.experimental import pallas as pl
from jax.experimental.pallas import tpu as pltpu
from jax.sharding import PartitionSpec as P

HEAD_DIM = 72
epsilon = 1e-06
MESH = pl.DeviceIdType.MESH
F32 = jnp.float32
BF16 = jnp.bfloat16


def normalize(rows):
    center = jnp.mean(rows, axis=-1, keepdims=True)
    centred = rows - center
    spread = jnp.mean(centred * centred, axis=-1, keepdims=True)
    inverse = lax.rsqrt(spread + epsilon)
    return (centred * inverse, inverse)


def norm_back(normed, inverse, upstream):
    mean_grad = jnp.mean(upstream, axis=-1, keepdims=True)
    mean_cross = jnp.mean(upstream * normed, axis=-1, keepdims=True)
    return (upstream - mean_grad - normed * mean_cross) * inverse


def dot(left, right):
    return jnp.dot(left, right, preferred_element_type=F32)


def dot_t(left, right):
    return lax.dot_general(left, right, (((1,), (1,)), ((), ())), preferred_element_type=F32)


def head_sums(product, same_head):
    high = product.astype(BF16)
    low = (product - high.astype(F32)).astype(BF16)
    return dot(high, same_head) + dot(low, same_head)


def kernel(dims, lat, mod, in_w, out_w, up_w, down_w, cot, same_head,
           res_out, lgrad_out, gin_out, gout_out, gup_out, gdown_out,
           LAT, COT, FIRST, BRANCH, SECOND, ATTG, QKV, DQKV, ATT, DACT, ACT, HG, XT, PART, keep,
           MID, MIDG, RESB, RESR, LGB, LGR, rsA, rsB, rsC, rsD,
           gdown, gup, gout, gin, ssem, rsem):
    Z, S, T, Fl, Pb, D, H, K = dims
    O = T // 2
    Fr = Fl * S
    R = Fr * Pb
    N = T * R
    z, s, t = lax.axis_index("dp"), lax.axis_index("seq"), lax.axis_index("tensor")
    o, inner = t // 2, lax.rem(t, 2)
    partner = {"tensor": o * 2 + 1 - inner}

    def outer(k):
        return lax.rem(o + k, O)

    def seq_peer(k):
        return lax.rem(s + k, S)

    def dp_peer(k):
        return lax.rem(z + k, Z)

    sends = []

    def send(src, dst, device):
        i = len(sends)
        copy = pltpu.make_async_remote_copy(
            src_ref=src, dst_ref=dst, send_sem=ssem.at[i], recv_sem=rsem.at[i],
            device_id=device, device_id_type=MESH)
        copy.start()
        sends.append(copy)
        return copy

    barrier = pltpu.get_barrier_semaphore()
    peers = [partner]
    peers += [{"tensor": outer(k) * 2 + inner} for k in range(1, O)]
    peers += [{"seq": seq_peer(k)} for k in range(1, S)]
    peers += [{"dp": dp_peer(k)} for k in range(1, Z)]
    for peer in peers:
        pl.semaphore_signal(barrier, inc=1, device_id=peer, device_id_type=MESH)
    pl.semaphore_wait(barrier, len(peers))

    def row(i):
        return mod[i : i + 1, :]

    def exchange_in(src, dst):
        copies = []
        for k in range(1, S):
            p = seq_peer(k)
            copies.append(send(src.at[:, p], dst.at[pl.ds(s * Fl, Fl)], {"seq": p}))
        dst[pl.ds(s * Fl, Fl)] = src[:, s]
        return copies

    def exchange_out(src, landed):
        copies = []
        for k in range(1, S):
            p = seq_peer(k)
            copies.append(send(src.at[pl.ds(p * Fl, Fl)], landed.at[k - 1], {"seq": p}))
        return copies

    def exchange_end(src, landed, out, copies):
        out[:, s] = src[pl.ds(s * Fl, Fl)]
        for k in range(1, S):
            copies[k - 1].wait_recv()
            out[:, lax.rem(s + S - k, S)] = landed[k - 1]

    def gather_start(buf):
        far = [send(buf.at[t], buf.at[t], {"tensor": outer(k) * 2 + inner}) for k in range(1, O)]
        near = [send(buf.at[t], buf.at[t], partner)]
        return far, near

    def gather_end(buf, state):
        far, near = state
        for k in range(1, O):
            far[k - 1].wait_recv()
            slot = lax.rem(o + O - k, O) * 2 + inner
            near.append(send(buf.at[slot], buf.at[slot], partner))
        for copy in near:
            copy.wait_recv()

    def scatter_start(compute, bufs):
        send1, recv1, send2, recv2 = bufs
        first = {}
        for k in list(range(1, O)) + [0]:
            PART[...] = compute(outer(k)).reshape(2, R, D)
            send1[k] = PART[1 - inner].astype(BF16)
            first[k] = send(send1.at[k], recv1.at[k], partner)
            keep[k] = PART[inner]
        second = []
        for k in range(1, O):
            first[k].wait_recv()
            send2[k - 1] = (keep[k] + recv1[k].astype(F32)).astype(BF16)
            second.append(send(send2.at[k - 1], recv2.at[k - 1], {"tensor": outer(k) * 2 + inner}))
        return first[0], second

    def scatter_end(bufs, state):
        send1, recv1, send2, recv2 = bufs
        state[0].wait_recv()
        total = keep[0] + recv1[0].astype(F32)
        for k in range(1, O):
            state[1][k - 1].wait_recv()
            total = total + recv2[k - 1].astype(F32)
        return total

    def pair(buf, i):
        both = buf[pl.ds(2 * i, 2)]
        return both.reshape(2 * R, both.shape[-1])

    def put_pair(buf, i, value):
        buf[pl.ds(2 * i, 2)] = value.reshape(2, R, value.shape[-1])

    def over_pairs(fn):
        def step(i, carry):
            fn(i)
            return carry
        lax.fori_loop(0, O, step, 0)

    def transpose_of(buf):
        for i in range(T):
            block = buf[i].T
            XT[:, :, i * R : (i + 1) * R] = block.reshape(Z, D // Z, R)

    def weight_start(right, bufs):
        local, rx, pz, rz = bufs
        def step(i, carry):
            value = dot(XT[i], right()).astype(BF16)
            local[i] = value.reshape(S, D // (Z * S), value.shape[-1])
            return carry
        lax.fori_loop(0, Z, step, 0)
        return [send(local.at[:, seq_peer(k)], rx.at[k - 1], {"seq": seq_peer(k)})
                for k in range(1, S)]

    def weight_mid(bufs, copies):
        local, rx, pz, rz = bufs
        for copy in copies:
            copy.wait_recv()
        def step(i, carry):
            total = local[i, s].astype(F32)
            for k in range(1, S):
                total = total + rx[k - 1, i].astype(F32)
            pz[i] = total.astype(BF16)
            return carry
        lax.fori_loop(0, Z, step, 0)
        return [send(pz.at[dp_peer(k)], rz.at[k - 1], {"dp": dp_peer(k)}) for k in range(1, Z)]

    def weight_end(bufs, copies):
        local, rx, pz, rz = bufs
        total = pz[z].astype(F32)
        for k in range(1, Z):
            copies[k - 1].wait_recv()
            total = total + rz[k - 1].astype(F32)
        return total.astype(BF16)

    lat_in = exchange_in(lat, LAT)
    cot_in = exchange_in(cot, COT)
    for copy in lat_in:
        copy.wait_recv()
    inputs = LAT[...].reshape(R, D).astype(F32)
    first_normed, first_inverse = normalize(inputs)
    FIRST[t] = (first_normed * (1.0 + row(1)) + row(0)).astype(BF16)
    first_state = gather_start(FIRST)
    for copy in cot_in:
        copy.wait_recv()
    BRANCH[t] = (row(5) * COT[...].reshape(R, D).astype(F32)).astype(BF16)
    branch_state = gather_start(BRANCH)
    gather_end(FIRST, first_state)

    def project(i):
        rows = pair(FIRST, i)
        for j in range(3):
            put_pair(QKV.at[j], i, dot(rows, in_w[j]).astype(BF16))
    over_pairs(project)

    scaling = 1.0 / math.sqrt(HEAD_DIM)

    def part(buf, j, i):
        return buf[j, i].astype(F32).reshape(Fr, Pb, H)

    def probabilities(q, k):
        scores = [head_sums((q * k[g : g + 1]).reshape(R, H), same_head[...]) * scaling for g in range(Fr)]
        highest = functools.reduce(jnp.maximum, scores)
        raised = [jnp.exp(score - highest) for score in scores]
        total = functools.reduce(jnp.add, raised)
        return [value / total for value in raised]

    def low(value):
        return value.astype(BF16).astype(F32)

    def attention(i, carry):
        q, k, v = part(QKV, 0, i), part(QKV, 1, i), part(QKV, 2, i)
        probs = probabilities(q, k)
        total = jnp.zeros((Fr, Pb, H), F32)
        for g in range(Fr):
            total = total + low(probs[g]).reshape(Fr, Pb, H) * v[g : g + 1]
        ATT[i] = total.reshape(R, H).astype(BF16)
        return carry
    lax.fori_loop(0, T, attention, 0)

    att_state = scatter_start(lambda i: dot(pair(ATT, i), out_w[...]), rsA)
    gather_end(BRANCH, branch_state)

    def branch_back(i):
        put_pair(DACT, i, dot_t(pair(BRANCH, i), down_w[...]))
    over_pairs(branch_back)
    midway = LAT[...].reshape(R, D).astype(F32) + row(2) * scatter_end(rsA, att_state)
    MID[...] = midway
    second_normed, second_inverse = normalize(midway)
    SECOND[t] = (second_normed * (1.0 + row(4)) + row(3)).astype(BF16)
    second_state = gather_start(SECOND)
    transpose_of(BRANCH)
    gather_end(SECOND, second_state)

    c = math.sqrt(2.0 / math.pi)

    def mlp(i):
        hidden = dot(pair(SECOND, i), up_w[...])
        square = hidden * hidden
        curve = jnp.tanh(c * (hidden + 0.044715 * square * hidden))
        put_pair(ACT, i, (0.5 * hidden * (1.0 + curve)).astype(BF16))
        slope = 0.5 * (1.0 + curve) + 0.5 * hidden * (1.0 - curve * curve) * (c * (1.0 + 3 * 0.044715 * square))
        put_pair(HG, i, (pair(DACT, i) * slope).astype(BF16))
    over_pairs(mlp)

    second_grad_state = scatter_start(lambda i: dot_t(pair(HG, i), up_w[...]), rsB)
    down_x = weight_start(lambda: ACT[...].reshape(N, K), gdown)
    second_grad = scatter_end(rsB, second_grad_state)
    second_normed, second_inverse = normalize(MID[...])
    midway_grad = COT[...].reshape(R, D).astype(F32) + norm_back(
        second_normed, second_inverse, second_grad * (1.0 + row(4)))
    MIDG[...] = midway_grad
    ATTG[t] = (row(2) * midway_grad).astype(BF16)
    attg_state = gather_start(ATTG)
    transpose_of(SECOND)
    up_x = weight_start(lambda: HG[...].reshape(N, K), gup)
    gather_end(ATTG, attg_state)
    transpose_of(ATTG)
    out_x = weight_start(lambda: ATT[...].reshape(N, H), gout)
    down_z = weight_mid(gdown, down_x)

    def attention_back(i, carry):
        q, k, v = part(QKV, 0, i), part(QKV, 1, i), part(QKV, 2, i)
        grad = dot_t(ATTG[i], out_w[...]).astype(BF16).astype(F32).reshape(Fr, Pb, H)
        probs = probabilities(q, k)
        prob_grads = [head_sums((grad * v[g : g + 1]).reshape(R, H), same_head[...]) for g in range(Fr)]
        cross = functools.reduce(jnp.add, [a * b for a, b in zip(probs, prob_grads)])
        dq = jnp.zeros((Fr, Pb, H), F32)
        for g in range(Fr):
            score = low(probs[g] * (prob_grads[g] - cross) * scaling).reshape(Fr, Pb, H)
            dq = dq + score * k[g : g + 1]
            DQKV[1, i, g * Pb : (g + 1) * Pb] = jnp.sum(score * q, axis=0).astype(BF16)
            DQKV[2, i, g * Pb : (g + 1) * Pb] = jnp.sum(
                low(probs[g]).reshape(Fr, Pb, H) * grad, axis=0).astype(BF16)
        DQKV[0, i] = dq.reshape(R, H).astype(BF16)
        return carry
    lax.fori_loop(0, T, attention_back, 0)

    def first_back(i):
        return sum(dot_t(pair(DQKV.at[j], i), in_w[j]) for j in range(3))
    first_grad_state = scatter_start(first_back, rsC)
    transpose_of(FIRST)
    in_x = [weight_start(lambda j=j: DQKV[j].reshape(N, H), gin[j]) for j in range(3)]
    up_z = weight_mid(gup, up_x)
    out_z = weight_mid(gout, out_x)
    first_grad = scatter_end(rsC, first_grad_state)
    first_normed, first_inverse = normalize(LAT[...].reshape(R, D).astype(F32))
    LGB[...] = (MIDG[...] + norm_back(first_normed, first_inverse, first_grad * (1.0 + row(1)))
                ).astype(BF16).reshape(Fr, Pb, D)
    lgrad_copies = exchange_out(LGB, LGR)

    result_state = scatter_start(lambda i: dot(pair(ACT, i), down_w[...]), rsD)
    in_z = [weight_mid(gin[j], in_x[j]) for j in range(3)]
    feedforward = scatter_end(rsD, result_state)
    RESB[...] = (MID[...] + row(5) * feedforward).astype(BF16).reshape(Fr, Pb, D)
    res_copies = exchange_out(RESB, RESR)
    exchange_end(LGB, LGR, lgrad_out, lgrad_copies)
    exchange_end(RESB, RESR, res_out, res_copies)
    gdown_out[...] = weight_end(gdown, down_z)
    gup_out[...] = weight_end(gup, up_z)
    for j in range(3):
        gin_out[j] = weight_end(gin[j], in_z[j])
    gout_out[...] = weight_end(gout, out_z)
    for copy in sends:
        copy.wait_send()


def body(sizes, latents, modulation, in_weight, out_weight, up_weight, down_weight, cotangent):
    Z, S, T = sizes
    _, Fl, Pl, D = latents.shape
    H, K = out_weight.shape[0], up_weight.shape[1]
    Pb, O = Pl // S, T // 2
    Fr = Fl * S
    R = Fr * Pb
    chunk = D // (Z * S)
    heads = jnp.arange(H) // HEAD_DIM
    same_head = (heads[:, None] == heads[None, :]).astype(BF16)

    def scatter_bufs():
        return (pltpu.VMEM((O, R, D), BF16), pltpu.VMEM((O, R, D), BF16),
                pltpu.VMEM((O - 1, R, D), BF16), pltpu.VMEM((O - 1, R, D), BF16))

    def weight_bufs(cols):
        return (pltpu.VMEM((Z, S, chunk, cols), BF16), pltpu.VMEM((S - 1, Z, chunk, cols), BF16),
                pltpu.VMEM((Z, chunk, cols), BF16), pltpu.VMEM((Z - 1, chunk, cols), BF16))

    full = pltpu.VMEM((T, R, D), BF16)
    tokens = pltpu.VMEM((Fr, Pb, D), BF16)
    landed = pltpu.VMEM((S - 1, Fl, Pb, D), BF16)
    copies = 2 * 4 * (S - 1 + O) + 4 * 2 * O + 6 * (S + Z)
    scratch = [
        tokens, tokens, full, full, full, full,
        pltpu.VMEM((3, T, R, H), BF16), pltpu.VMEM((3, T, R, H), BF16),
        pltpu.VMEM((T, R, H), BF16), pltpu.VMEM((T, R, K), F32),
        pltpu.VMEM((T, R, K), BF16), pltpu.VMEM((T, R, K), BF16),
        pltpu.VMEM((Z, D // Z, T * R), BF16), pltpu.VMEM((2, R, D), F32),
        pltpu.VMEM((O, R, D), F32),
        pltpu.VMEM((R, D), F32), pltpu.VMEM((R, D), F32),
        tokens, landed, tokens, landed,
        scatter_bufs(), scatter_bufs(), scatter_bufs(), scatter_bufs(),
        weight_bufs(K), weight_bufs(K), weight_bufs(H), tuple(weight_bufs(H) for _ in range(3)),
        pltpu.SemaphoreType.DMA((copies,)), pltpu.SemaphoreType.DMA((copies,)),
    ]
    vmem = pl.BlockSpec(memory_space=pltpu.VMEM)
    shape = jax.ShapeDtypeStruct
    outs = pl.pallas_call(
        functools.partial(kernel, (Z, S, T, Fl, Pb, D, H, K)),
        out_shape=(
            shape((Fl, S, Pb, D), BF16), shape((Fl, S, Pb, D), BF16),
            shape((3, chunk, H), BF16), shape((chunk, H), BF16),
            shape((chunk, K), BF16), shape((chunk, K), BF16)),
        in_specs=[vmem] * 8,
        out_specs=(vmem,) * 6,
        scratch_shapes=scratch,
        compiler_params=pltpu.CompilerParams(
            collective_id=0, has_side_effects=True, vmem_limit_bytes=67043328),
    )(latents.reshape(Fl, S, Pb, D), modulation[0], in_weight.transpose(1, 0, 2), out_weight,
      up_weight, down_weight, cotangent.reshape(Fl, S, Pb, D), same_head)
    res, lgrad, gin, gout, gup, gdown = outs
    return (res.reshape(1, Fl, Pl, D), lgrad.reshape(1, Fl, Pl, D), gin.transpose(1, 0, 2),
            gout.T, gup, gdown.T)


def solution(mesh):
    placed = (
        P("dp", "seq", "tensor", None),
        P("dp", None, None),
        P(None, None, "tensor"),
        P("tensor", None),
        P(None, "tensor"),
        P("tensor", None),
        P("dp", "seq", "tensor", None),
    )
    sizes = (mesh.shape["dp"], mesh.shape["seq"], mesh.shape["tensor"])
    return jax.shard_map(
        functools.partial(body, sizes),
        mesh=mesh,
        in_specs=placed,
        out_specs=(
            P("dp", "seq", "tensor", None),
            P("dp", "seq", "tensor", None),
            P(("dp", "seq"), None, "tensor"),
            P("tensor", ("dp", "seq")),
            P(("dp", "seq"), "tensor"),
            P("tensor", ("dp", "seq")),
        ),
        check_vma=False,
    )
```
